128 devices in a mesh: row: 4 (over z_hi, core), col: 32 (over z_lo, y, x).
Axes of the slice: x: 4, y: 4, z: 4 (z_hi: 2, z_lo: 2; z = z_hi * 2 + z_lo), core: 2. Of those that a mesh axis runs over, the one named last changes fastest.
Arguments:
- tensor: float32 [1024, 512, 1024], P('row', 'col'), may hold values from -6 to 6
- start_basis: float32 [1024, 256], P(('row', 'col')), may hold values from -6 to 6
Outputs:
- scaled_basis: float32 [1024, 256], P(('row', 'col'))
- core: float32 [1024, 512, 256], P('row', 'col')
The draws below stay inside these ranges and needn't reach their ends.
All inputs are finite; a program needn't handle non-finite values.
Results may differ from the reference program's by a relative error of at most 0.0003.
Values sent between devices are 32-bit elements; how exact they have to be, the bound alone decides.
No kernel may reach another device: no remote copies, remote signals or barrier semaphores. Data moves between devices by JAX's collectives and lax.ppermute only.
A program may use at most 128 MiB of HBM per device.

```python
import math
import jax
import jax.numpy as jnp
from jax import lax

N2 = 1024
K = 256
PASSES = 2
N1 = 1024
N3 = 512


def raised(drawn, own_key, source, target, shards_of, factor):
    def block_of(axis_at):
        return (jnp.arange(drawn.shape[axis_at]) // (drawn.shape[axis_at] // shards_of)).reshape((-1,) + (1,) * (drawn.ndim - 1 - axis_at))

    first = jax.random.permutation(own_key, shards_of)[block_of(target)]
    far = (block_of(target) + shards_of // 2) % shards_of
    return jnp.where((block_of(source) == first) | (block_of(source) == far), factor * drawn, drawn)


def block_levels(stream_key, dims, split, smallest, high):
    level, own = 1.0, jax.random.fold_in(stream_key, 6)
    for axis_at, shards_of in split:
        draws = jnp.exp(jax.random.uniform(jax.random.fold_in(own, axis_at), (shards_of,), jnp.float32, smallest / len(split), high / len(split)))
        level = level * jnp.repeat(draws, dims[axis_at] // shards_of).reshape([-1 if axis == axis_at else 1 for axis in range(len(dims))])
    return level


def bell_draw(stream_key, extent, scale, reach, cuts=(), kind=jnp.bfloat16):
    level = block_levels(stream_key, extent, cuts, -0.22, 0.18) if cuts else 1.0
    result = jax.random.normal(stream_key, extent, jnp.float32) * scale * level
    return jnp.minimum(jnp.maximum(result, -reach), reach).astype(kind)


def noise_with(own_key, extent, scale, reach, shards, heavy, kind=jnp.bfloat16):
    result = scale * jax.random.normal(own_key, extent, jnp.float32)
    if shards:
        result = result * block_levels(own_key, extent, shards, -0.22, 0.18)
    return jnp.clip(raised(result, jax.random.fold_in(own_key, 3), *heavy), -reach, reach).astype(kind)


def setup_inputs(seed: int = 0) -> dict:
    key_of = jax.random.split(jax.random.key(seed), 3)
    tensor = noise_with(key_of[0], (N1, N3, N2), 1.0, 6.0, ((0, 4), (1, 32)), (1, 2, 32, 2.75), jnp.float32)
    start_basis = bell_draw(key_of[1], (N2, K), 1.0, 6.0, ((0, 128),), jnp.float32)
    return {"tensor": tensor, "start_basis": start_basis}


def orthonormal(tall_block):
    gram_part = jnp.dot(tall_block.T.astype(jnp.float32), tall_block.astype(jnp.float32), precision=lax.Precision.HIGHEST, preferred_element_type=jnp.float32)
    cholesky_low = jnp.linalg.cholesky(gram_part)
    return jax.scipy.linalg.solve_triangular(cholesky_low, tall_block.T, lower=True).T

def reference(tensor, start_basis):
    subspace = start_basis
    for repeat in range(PASSES):
        coefficients = jnp.einsum('ikj,jr->ikr', tensor, subspace, precision=lax.Precision.HIGHEST)
        product = jnp.einsum('ikj,ikr->jr', tensor, coefficients, precision=lax.Precision.HIGHEST)
        subspace = orthonormal(product)
    core = jnp.einsum('ikj,jr->ikr', tensor, subspace, precision=lax.Precision.HIGHEST)
    return (math.sqrt(N2) * subspace, core)
```

```python
import functools

import jax
import jax.numpy as jnp
from jax import lax
from jax.experimental import pallas as pl
from jax.experimental.pallas import tpu as pltpu
from jax.sharding import Mesh
from jax.sharding import PartitionSpec as P

PASSES = 2
N2 = 1024
K = 256
BLK = 256
NB = N2 // BLK
PACKED = BLK * NB * (NB + 1) // 2
LANES = 128
CHIPS = 64
OWN = PACKED // CHIPS
START = 8
PAY = OWN + 2 * START
GRAM_ROWS = 512
CORE_ROWS = 512
GROUP = 8
F32 = jnp.float32
BF16 = jnp.bfloat16
NN = (((1,), (0,)), ((), ()))
NT = (((1,), (1,)), ((), ()))
TN = (((0,), (0,)), ((), ()))


def mm(a, b, dims=NN):
    return lax.dot_general(a, b, dims, preferred_element_type=F32)


def split2(x):
    hi = x.astype(BF16)
    return hi, (x - hi.astype(F32)).astype(BF16)


def split3(x):
    hi = x.astype(BF16)
    rest = x - hi.astype(F32)
    mid = rest.astype(BF16)
    return hi, mid, (rest - mid.astype(F32)).astype(BF16)


def mm3(a, b, dims=NN):
    ah, al = split2(a)
    bh, bl = split2(b)
    return mm(ah, bh, dims) + (mm(ah, bl, dims) + mm(al, bh, dims))


def mm6(a, b, dims=NN):
    ah, am, al = split3(a)
    bh, bm, bl = split3(b)
    small = mm(am, bm, dims) + (mm(ah, bl, dims) + mm(al, bh, dims))
    return mm(ah, bh, dims) + ((mm(ah, bm, dims) + mm(am, bh, dims)) + small)


def gram_kernel(core_ref, slab_ref, keep_ref, send_ref, acc_ref):
    step = pl.program_id(0)

    @pl.when(step == 0)
    def _():
        acc_ref[...] = jnp.zeros_like(acc_ref)

    hi, lo = split2(slab_ref[...])
    hi_t, lo_t = hi.T, lo.T
    for b in range(NB):
        cols = slice(b * BLK, (b + 1) * BLK)
        hb, lb = hi[:, cols], lo[:, cols]
        top = b * BLK
        row = BLK * b * (b + 1) // 2
        if b:
            part = mm(hi_t[:top], hb) + mm(hi_t[:top], lb) + mm(lo_t[:top], hb)
            acc_ref[0, row : row + top] += part[:, :LANES]
            acc_ref[1, row : row + top] += part[:, LANES:]
        part = mm(hi_t[cols], hb) + mm(hi_t[cols], lb + lb)
        acc_ref[0, row + top : row + top + BLK] += part[:, :LANES]
        acc_ref[1, row + top : row + top + BLK] += part[:, LANES:]

    @pl.when(step == pl.num_programs(0) - 1)
    def _():
        core = core_ref[0]
        keep_ref[...] = acc_ref[core]
        send_ref[...] = acc_ref[1 - core]


def packed_gram(core, slab):
    rows = slab.shape[0]
    half = jax.ShapeDtypeStruct((PACKED, LANES), F32)
    whole = pl.BlockSpec((PACKED, LANES), lambda i, c: (0, 0))
    return pl.pallas_call(
        gram_kernel,
        out_shape=(half, half),
        grid_spec=pltpu.PrefetchScalarGridSpec(
            num_scalar_prefetch=1,
            grid=(rows // GRAM_ROWS,),
            in_specs=[pl.BlockSpec((GRAM_ROWS, N2), lambda i, c: (i, 0))],
            out_specs=(whole, whole),
            scratch_shapes=[pltpu.VMEM((2, PACKED, LANES), F32)],
        ),
        compiler_params=pltpu.CompilerParams(
            dimension_semantics=("arbitrary",), vmem_limit_bytes=48 << 20
        ),
        name="packed_gram",
    )(core, slab)


def join_kernel(parts_ref, start_ref, out_ref):
    total = jnp.sum(parts_ref[...], axis=0)
    pay = jnp.concatenate([total, start_ref[:, :LANES], start_ref[:, LANES:]], axis=0)
    out_ref[...] = jnp.broadcast_to(pay[None], out_ref.shape)


def joined(parts, start):
    return pl.pallas_call(
        join_kernel,
        out_shape=jax.ShapeDtypeStruct((CHIPS, PAY, LANES), F32),
        name="join",
    )(parts, start)


def eliminate(aug_ref):
    rows8 = lax.broadcasted_iota(jnp.int32, (GROUP, LANES), 0)
    lane = lax.broadcasted_iota(jnp.int32, (1, K), 1)

    def group(g, carry):
        base = g * GROUP
        panel = aug_ref[pl.ds(base, GROUP), :]
        tile = jnp.where(base < LANES, panel[:, :LANES], panel[:, LANES : 2 * LANES])
        tile = pltpu.roll(tile, (LANES - base % LANES) % LANES, 1)
        cols = [jnp.broadcast_to(tile[:, t : t + 1], (GROUP, LANES)) for t in range(GROUP)]
        parts = [panel[:, i * LANES : (i + 1) * LANES] for i in range(2 * K // LANES)]
        inv = jnp.zeros((GROUP, LANES), F32)
        for t in range(GROUP):
            pivot = jnp.broadcast_to(cols[t][t : t + 1], (GROUP, LANES))
            recip = 1.0 / pivot
            mult = jnp.where(rows8 > t, cols[t] * recip, 0.0)
            inv = jnp.where(rows8 == t, recip, inv)
            for s in range(t + 1, GROUP):
                cols[s] = cols[s] - mult * jnp.broadcast_to(cols[s][t : t + 1], (GROUP, LANES))
            parts = [p - mult * jnp.broadcast_to(p[t : t + 1], (GROUP, LANES)) for p in parts]
        panel = jnp.concatenate(parts, axis=1)
        aug_ref[pl.ds(base, GROUP), :] = panel
        lower = panel[:, :K] * jnp.concatenate([inv] * (K // LANES), axis=1)
        lower = jnp.where(lane >= base + GROUP, lower, 0.0)
        lh, lm, ll = split3(lower)
        ph, pm, plow = split3(panel)
        left = jnp.concatenate([lh, lh, lm, lm, lh, ll], axis=0)
        right = jnp.concatenate([ph, pm, ph, pm, plow, ph], axis=0)
        for c in range(0, K, 64):

            @pl.when(c + 64 > base + GROUP)
            def _():
                aug_ref[c : c + 64, :] -= mm(left[:, c : c + 64], right, TN)

        return carry

    lax.fori_loop(0, K // GROUP, group, 0)


def passes_kernel(meta_ref, mine_ref, other_ref, own_ref, basis_ref, gh_ref, gl_ref, aug_ref):
    core = meta_ref[0]
    slot = meta_ref[1]
    quarter = CHIPS // 2 * START

    def place(h, ref):
        packed = ref[:, :OWN, :].reshape(PACKED, LANES)
        for b in range(NB):
            for a in range(b):
                row = BLK * (b * (b + 1) // 2 + a)
                block = packed[row : row + BLK]
                hi, lo = split2(block)
                at = b * BLK + h * LANES
                gh_ref[a * BLK : (a + 1) * BLK, at : at + LANES] = hi
                gl_ref[a * BLK : (a + 1) * BLK, at : at + LANES] = lo
                hi, lo = split2(block.T)
                gh_ref[at : at + LANES, a * BLK : (a + 1) * BLK] = hi
                gl_ref[at : at + LANES, a * BLK : (a + 1) * BLK] = lo

    def place_diagonal(left, right):
        for b in range(NB):
            row = BLK * (b * (b + 1) // 2 + b)
            block = jnp.concatenate(
                [r[:, :OWN, :].reshape(PACKED, LANES)[row : row + BLK] for r in (left, right)], axis=1
            )
            hi, lo = split2(0.5 * (block + block.T))
            at = slice(b * BLK, (b + 1) * BLK)
            gh_ref[at, at] = hi
            gl_ref[at, at] = lo

    def place_start(h, ref):
        for half in range(2):
            chips = slice(half * CHIPS // 2, (half + 1) * CHIPS // 2)
            at = half * 2 * quarter + h * quarter
            for side in range(2):
                rows = ref[chips, OWN + side * START : OWN + (side + 1) * START, :]
                basis_ref[at : at + quarter, side * LANES : (side + 1) * LANES] = rows.reshape(quarter, LANES)

    def unpack(left, right):
        for h, ref in enumerate((left, right)):
            place(h, ref)
            place_start(h, ref)
        place_diagonal(left, right)

    @pl.when(core == 0)
    def _():
        unpack(mine_ref, other_ref)

    @pl.when(core == 1)
    def _():
        unpack(other_ref, mine_ref)

    diag = lax.broadcasted_iota(jnp.int32, (K, K), 0) == lax.broadcasted_iota(jnp.int32, (K, K), 1)

    def one_pass(repeat, carry):
        bh, bl = split2(basis_ref[...])
        product = mm(gh_ref[...], bh) + (mm(gh_ref[...], bl) + mm(gl_ref[...], bh))
        aug_ref[:, :K] = mm6(product, product, TN)
        aug_ref[:, K:] = jnp.where(diag, 1.0, 0.0)
        eliminate(aug_ref)
        pivots = jnp.sum(jnp.where(diag, aug_ref[:, :K], 0.0), axis=1, keepdims=True)
        inverse = aug_ref[:, K:] * lax.rsqrt(pivots)
        basis_ref[...] = mm6(product, inverse, NT)
        return carry

    lax.fori_loop(0, PASSES, one_pass, 0)
    own_ref[...] = basis_ref[pl.ds(slot * START, START), :] * (float(N2) ** 0.5)


def passes(meta, mine, other):
    vmem = pl.BlockSpec(memory_space=pltpu.VMEM)
    return pl.pallas_call(
        passes_kernel,
        out_shape=(
            jax.ShapeDtypeStruct((START, K), F32),
            jax.ShapeDtypeStruct((N2, K), F32),
        ),
        in_specs=[pl.BlockSpec(memory_space=pltpu.SMEM), vmem, vmem],
        out_specs=(vmem, vmem),
        scratch_shapes=[
            pltpu.VMEM((N2, N2), BF16),
            pltpu.VMEM((N2, N2), BF16),
            pltpu.VMEM((K, 2 * K), F32),
        ],
        compiler_params=pltpu.CompilerParams(vmem_limit_bytes=48 << 20),
        name="passes",
    )(meta, mine, other)


def core_kernel(slab_ref, basis_ref, out_ref):
    out_ref[...] = mm3(slab_ref[...], basis_ref[...])


def core_block(slab, basis):
    rows = slab.shape[0]
    return pl.pallas_call(
        core_kernel,
        out_shape=jax.ShapeDtypeStruct((rows, K), F32),
        grid=(rows // CORE_ROWS,),
        in_specs=[
            pl.BlockSpec((CORE_ROWS, N2), lambda i: (i, 0)),
            pl.BlockSpec((N2, K), lambda i: (0, 0)),
        ],
        out_specs=pl.BlockSpec((CORE_ROWS, K), lambda i: (i, 0)),
        compiler_params=pltpu.CompilerParams(
            dimension_semantics=("arbitrary",), vmem_limit_bytes=48 << 20
        ),
        name="core_block",
    )(slab, basis)


CHIP_AXES = ("zhi", "zlo", "y", "x")


def swap_cores(x):
    return lax.ppermute(x, "core", [(0, 1), (1, 0)])


def exchange(x):
    return lax.all_to_all(x, CHIP_AXES, split_axis=0, concat_axis=0)


def body(tensor, start_basis):
    core = lax.axis_index("core")
    col = (lax.axis_index("zlo") * 4 + lax.axis_index("y")) * 4 + lax.axis_index("x")
    slot = (lax.axis_index("zhi") * 2 + core) * 32 + col
    slab = tensor.reshape(-1, N2)
    keep, send = packed_gram(core.reshape(1), slab)
    chip = (keep + swap_cores(send)).reshape(CHIPS, OWN, LANES)
    mine = exchange(joined(exchange(chip), start_basis))
    own, basis = passes(jnp.stack([core, slot]), mine, swap_cores(mine))
    core_out = core_block(slab, basis)
    return own, core_out.reshape(tensor.shape[0], tensor.shape[1], K)


def solution(mesh):
    split = Mesh(mesh.devices.reshape(2, 2, 2, 4, 4), ("zhi", "core", "zlo", "y", "x"))
    row, col = ("zhi", "core"), ("zlo", "y", "x")
    return jax.shard_map(
        body,
        mesh=split,
        in_specs=(P(row, col, None), P(row + col, None)),
        out_specs=(P(row + col, None), P(row, col, None)),
        check_vma=False,
    )
```

```python
import functools

import jax
import jax.numpy as jnp
from jax import lax
from jax.experimental import pallas as pl
from jax.experimental.pallas import tpu as pltpu
from jax.sharding import Mesh
from jax.sharding import PartitionSpec as P

PASSES = 2
N2 = 1024
K = 256
BLK = 256
NB = N2 // BLK
PACKED = BLK * NB * (NB + 1) // 2
LANES = 128
CHIPS = 64
OWN = PACKED // CHIPS
START = 8
PAY = OWN + 2 * START
GRAM_ROWS = 512
CORE_ROWS = 512
GROUP = 16
F32 = jnp.float32
BF16 = jnp.bfloat16
NN = (((1,), (0,)), ((), ()))
NT = (((1,), (1,)), ((), ()))
TN = (((0,), (0,)), ((), ()))


def mm(a, b, dims=NN):
    return lax.dot_general(a, b, dims, preferred_element_type=F32)


def split2(x):
    hi = x.astype(BF16)
    return hi, (x - hi.astype(F32)).astype(BF16)


def split3(x):
    hi = x.astype(BF16)
    rest = x - hi.astype(F32)
    mid = rest.astype(BF16)
    return hi, mid, (rest - mid.astype(F32)).astype(BF16)


def mm3(a, b, dims=NN):
    ah, al = split2(a)
    bh, bl = split2(b)
    return mm(ah, bh, dims) + (mm(ah, bl, dims) + mm(al, bh, dims))


def mm6(a, b, dims=NN):
    ah, am, al = split3(a)
    bh, bm, bl = split3(b)
    small = mm(am, bm, dims) + (mm(ah, bl, dims) + mm(al, bh, dims))
    return mm(ah, bh, dims) + ((mm(ah, bm, dims) + mm(am, bh, dims)) + small)


def gram_kernel(core_ref, slab_ref, keep_ref, send_ref, acc_ref):
    step = pl.program_id(0)

    @pl.when(step == 0)
    def _():
        acc_ref[...] = jnp.zeros_like(acc_ref)

    hi, lo = split2(slab_ref[...])
    hi_t, lo_t = hi.T, lo.T
    for b in range(NB):
        cols = slice(b * BLK, (b + 1) * BLK)
        hb, lb = hi[:, cols], lo[:, cols]
        top = b * BLK
        row = BLK * b * (b + 1) // 2
        if b:
            part = mm(hi_t[:top], hb) + mm(hi_t[:top], lb) + mm(lo_t[:top], hb)
            acc_ref[0, row : row + top] += part[:, :LANES]
            acc_ref[1, row : row + top] += part[:, LANES:]
        part = mm(hi_t[cols], hb) + mm(hi_t[cols], lb + lb)
        acc_ref[0, row + top : row + top + BLK] += part[:, :LANES]
        acc_ref[1, row + top : row + top + BLK] += part[:, LANES:]

    @pl.when(step == pl.num_programs(0) - 1)
    def _():
        core = core_ref[0]
        keep_ref[...] = acc_ref[core]
        send_ref[...] = acc_ref[1 - core]


def packed_gram(core, slab):
    rows = slab.shape[0]
    half = jax.ShapeDtypeStruct((PACKED, LANES), F32)
    whole = pl.BlockSpec((PACKED, LANES), lambda i, c: (0, 0))
    return pl.pallas_call(
        gram_kernel,
        out_shape=(half, half),
        grid_spec=pltpu.PrefetchScalarGridSpec(
            num_scalar_prefetch=1,
            grid=(rows // GRAM_ROWS,),
            in_specs=[pl.BlockSpec((GRAM_ROWS, N2), lambda i, c: (i, 0))],
            out_specs=(whole, whole),
            scratch_shapes=[pltpu.VMEM((2, PACKED, LANES), F32)],
        ),
        compiler_params=pltpu.CompilerParams(
            dimension_semantics=("arbitrary",), vmem_limit_bytes=48 << 20
        ),
        name="packed_gram",
    )(core, slab)


def join_kernel(parts_ref, start_ref, out_ref):
    total = jnp.sum(parts_ref[...], axis=0)
    pay = jnp.concatenate([total, start_ref[:, :LANES], start_ref[:, LANES:]], axis=0)
    out_ref[...] = jnp.broadcast_to(pay[None], out_ref.shape)


def joined(parts, start):
    return pl.pallas_call(
        join_kernel,
        out_shape=jax.ShapeDtypeStruct((CHIPS, PAY, LANES), F32),
        name="join",
    )(parts, start)


def eliminate(aug_ref):
    sub = lax.broadcasted_iota(jnp.int32, (8, LANES), 0)
    lane = lax.broadcasted_iota(jnp.int32, (1, LANES), 1)
    halves = GROUP // 8
    ones = jnp.ones((8, LANES), F32)
    for base in range(0, K, GROUP):
        first = base // LANES
        off = base % LANES
        tiles = range(first, first + 3)
        rows = [
            [aug_ref[base + 8 * v : base + 8 * v + 8, i * LANES : (i + 1) * LANES] for i in tiles]
            for v in range(halves)
        ]
        cols = [
            [jnp.broadcast_to(rows[v][0][:, off + t : off + t + 1], (8, LANES)) for t in range(GROUP)]
            for v in range(halves)
        ]
        inv = [ones for _ in range(halves)]
        for t in range(GROUP):
            vt, st = t // 8, t % 8
            pivot_col = [jnp.broadcast_to(cols[vt][s][st : st + 1], (8, LANES)) for s in range(t, GROUP)]
            pivot_row = [jnp.broadcast_to(r[st : st + 1], (8, LANES)) for r in rows[vt]]
            recip = 1.0 / pivot_col[0]
            inv[vt] = jnp.where(sub == st, recip, inv[vt])
            for v in range(vt, halves):
                mult = cols[v][t] * recip
                if v == vt:
                    mult = jnp.where(sub > st, mult, 0.0)
                for s in range(t + 1, GROUP):
                    cols[v][s] = cols[v][s] - mult * pivot_col[s - t]
                rows[v] = [r - mult * p for r, p in zip(rows[v], pivot_row)]
        upper = jnp.concatenate([jnp.concatenate(r, axis=1) for r in rows], axis=0)
        for v in range(halves):
            for i in range(first + 1):
                at = K + i * LANES
                aug_ref[base + 8 * v : base + 8 * v + 8, at : at + LANES] = rows[v][i + 2 - first] * jnp.sqrt(inv[v])
        if base + GROUP == K:
            break
        lower = jnp.concatenate(
            [jnp.concatenate([rows[v][i - first] * inv[v] for i in range(first, 2)], axis=1) for v in range(halves)],
            axis=0,
        )
        lh, lm, ll = split3(lower)
        uh, um, ul = split3(upper)
        left = jnp.concatenate([lh, lh, lm, lm, lh, ll], axis=0).T
        right = jnp.concatenate([uh, um, uh, um, ul, uh], axis=0)
        start = base + GROUP
        at = slice(first * LANES, (first + 3) * LANES)
        for lo, hi in ((start, start + GROUP), (start + GROUP, K)):
            if lo < hi:
                shift = first * LANES
                aug_ref[lo:hi, at] = aug_ref[lo:hi, at] - mm(left[lo - shift : hi - shift], right)


def passes_kernel(meta_ref, mine_ref, other_ref, own_ref, basis_ref, gh_ref, gl_ref, aug_ref):
    core = meta_ref[0]
    slot = meta_ref[1]
    quarter = CHIPS // 2 * START

    def place(h, ref):
        packed = ref[:, :OWN, :].reshape(PACKED, LANES)
        for b in range(NB):
            for a in range(b):
                row = BLK * (b * (b + 1) // 2 + a)
                block = packed[row : row + BLK]
                hi, lo = split2(block)
                at = b * BLK + h * LANES
                gh_ref[a * BLK : (a + 1) * BLK, at : at + LANES] = hi
                gl_ref[a * BLK : (a + 1) * BLK, at : at + LANES] = lo
                hi, lo = split2(block.T)
                gh_ref[at : at + LANES, a * BLK : (a + 1) * BLK] = hi
                gl_ref[at : at + LANES, a * BLK : (a + 1) * BLK] = lo

    def place_diagonal(left, right):
        for b in range(NB):
            row = BLK * (b * (b + 1) // 2 + b)
            block = jnp.concatenate(
                [r[:, :OWN, :].reshape(PACKED, LANES)[row : row + BLK] for r in (left, right)], axis=1
            )
            hi, lo = split2(0.5 * (block + block.T))
            at = slice(b * BLK, (b + 1) * BLK)
            gh_ref[at, at] = hi
            gl_ref[at, at] = lo

    def place_start(h, ref):
        for half in range(2):
            chips = slice(half * CHIPS // 2, (half + 1) * CHIPS // 2)
            at = half * 2 * quarter + h * quarter
            for side in range(2):
                rows = ref[chips, OWN + side * START : OWN + (side + 1) * START, :]
                basis_ref[at : at + quarter, side * LANES : (side + 1) * LANES] = rows.reshape(quarter, LANES)

    def unpack(left, right):
        for h, ref in enumerate((left, right)):
            place(h, ref)
            place_start(h, ref)
        place_diagonal(left, right)

    @pl.when(core == 0)
    def _():
        unpack(mine_ref, other_ref)

    @pl.when(core == 1)
    def _():
        unpack(other_ref, mine_ref)

    diag = lax.broadcasted_iota(jnp.int32, (K, K), 0) == lax.broadcasted_iota(jnp.int32, (K, K), 1)

    def one_pass(repeat, carry):
        bh, bl = split2(basis_ref[...])
        product = mm(gh_ref[...], bh) + (mm(gh_ref[...], bl) + mm(gl_ref[...], bh))
        aug_ref[:, :K] = mm6(product, product, TN)
        aug_ref[:, K:] = jnp.where(diag, 1.0, 0.0)
        eliminate(aug_ref)
        inverse = aug_ref[:, K:]
        basis_ref[...] = mm6(product, inverse, NT)
        return carry

    lax.fori_loop(0, PASSES, one_pass, 0)
    own_ref[...] = basis_ref[pl.ds(slot * START, START), :] * (float(N2) ** 0.5)


def passes(meta, mine, other):
    vmem = pl.BlockSpec(memory_space=pltpu.VMEM)
    return pl.pallas_call(
        passes_kernel,
        out_shape=(
            jax.ShapeDtypeStruct((START, K), F32),
            jax.ShapeDtypeStruct((N2, K), F32),
        ),
        in_specs=[pl.BlockSpec(memory_space=pltpu.SMEM), vmem, vmem],
        out_specs=(vmem, vmem),
        scratch_shapes=[
            pltpu.VMEM((N2, N2), BF16),
            pltpu.VMEM((N2, N2), BF16),
            pltpu.VMEM((K, 2 * K), F32),
        ],
        compiler_params=pltpu.CompilerParams(vmem_limit_bytes=48 << 20),
        name="passes",
    )(meta, mine, other)


def core_kernel(slab_ref, basis_ref, out_ref):
    out_ref[...] = mm3(slab_ref[...], basis_ref[...])


def core_block(slab, basis):
    rows = slab.shape[0]
    return pl.pallas_call(
        core_kernel,
        out_shape=jax.ShapeDtypeStruct((rows, K), F32),
        grid=(rows // CORE_ROWS,),
        in_specs=[
            pl.BlockSpec((CORE_ROWS, N2), lambda i: (i, 0)),
            pl.BlockSpec((N2, K), lambda i: (0, 0)),
        ],
        out_specs=pl.BlockSpec((CORE_ROWS, K), lambda i: (i, 0)),
        compiler_params=pltpu.CompilerParams(
            dimension_semantics=("arbitrary",), vmem_limit_bytes=48 << 20
        ),
        name="core_block",
    )(slab, basis)


CHIP_AXES = ("zhi", "zlo", "y", "x")


def swap_cores(x):
    return lax.ppermute(x, "core", [(0, 1), (1, 0)])


def exchange(x):
    return lax.all_to_all(x, CHIP_AXES, split_axis=0, concat_axis=0)


def body(tensor, start_basis):
    core = lax.axis_index("core")
    col = (lax.axis_index("zlo") * 4 + lax.axis_index("y")) * 4 + lax.axis_index("x")
    slot = (lax.axis_index("zhi") * 2 + core) * 32 + col
    slab = tensor.reshape(-1, N2)
    keep, send = packed_gram(core.reshape(1), slab)
    chip = (keep + swap_cores(send)).reshape(CHIPS, OWN, LANES)
    mine = exchange(joined(exchange(chip), start_basis))
    own, basis = passes(jnp.stack([core, slot]), mine, swap_cores(mine))
    core_out = core_block(slab, basis)
    return own, core_out.reshape(tensor.shape[0], tensor.shape[1], K)


def solution(mesh):
    split = Mesh(mesh.devices.reshape(2, 2, 2, 4, 4), ("zhi", "core", "zlo", "y", "x"))
    row, col = ("zhi", "core"), ("zlo", "y", "x")
    return jax.shard_map(
        body,
        mesh=split,
        in_specs=(P(row, col, None), P(row + col, None)),
        out_specs=(P(row + col, None), P(row, col, None)),
        check_vma=False,
    )
```

```python
import jax
import jax.numpy as jnp
from jax import lax
from jax.experimental import pallas as pl
from jax.experimental.pallas import tpu as pltpu
from jax.sharding import Mesh
from jax.sharding import PartitionSpec as P


PASSES = 2
N2 = 1024
K = 256
BLK = 256
NB = N2 // BLK
PACKED = BLK * NB * (NB + 1) // 2
LANES = 128
CHIPS = 64
OWN = PACKED // CHIPS
START = 8
GRAM_ROWS = 512
CORE_ROWS = 512
GROUP = 16
F32 = jnp.float32
BF16 = jnp.bfloat16
NN = (((1,), (0,)), ((), ()))
NT = (((1,), (1,)), ((), ()))
TN = (((0,), (0,)), ((), ()))


def mm(a, b, dims=NN):
    return lax.dot_general(a, b, dims, preferred_element_type=F32)


def split2(x):
    hi = x.astype(BF16)
    return hi, (x - hi.astype(F32)).astype(BF16)


def split3(x):
    hi = x.astype(BF16)
    rest = x - hi.astype(F32)
    mid = rest.astype(BF16)
    return hi, mid, (rest - mid.astype(F32)).astype(BF16)


def mm3(a, b, dims=NN):
    ah, al = split2(a)
    bh, bl = split2(b)
    return mm(ah, bh, dims) + (mm(ah, bl, dims) + mm(al, bh, dims))


def mm6(a, b, dims=NN):
    ah, am, al = split3(a)
    bh, bm, bl = split3(b)
    small = mm(am, bm, dims) + (mm(ah, bl, dims) + mm(al, bh, dims))
    return mm(ah, bh, dims) + ((mm(ah, bm, dims) + mm(am, bh, dims)) + small)


def gram_kernel(core_ref, slab_ref, keep_ref, send_ref, acc_ref):
    step = pl.program_id(0)

    @pl.when(step == 0)
    def _():
        acc_ref[...] = jnp.zeros_like(acc_ref)

    hi, lo = split2(slab_ref[...])
    hi_t, lo_t = hi.T, lo.T
    for b in range(NB):
        cols = slice(b * BLK, (b + 1) * BLK)
        hb, lb = hi[:, cols], lo[:, cols]
        top = b * BLK
        row = BLK * b * (b + 1) // 2
        if b:
            part = mm(hi_t[:top], hb) + mm(hi_t[:top], lb) + mm(lo_t[:top], hb)
            acc_ref[0, row : row + top] += part[:, :LANES]
            acc_ref[1, row : row + top] += part[:, LANES:]
        part = mm(hi_t[cols], hb) + mm(hi_t[cols], lb + lb)
        acc_ref[0, row + top : row + top + BLK] += part[:, :LANES]
        acc_ref[1, row + top : row + top + BLK] += part[:, LANES:]

    @pl.when(step == pl.num_programs(0) - 1)
    def _():
        core = core_ref[0]
        keep_ref[...] = acc_ref[core]
        send_ref[...] = acc_ref[1 - core]


def packed_gram(core, slab):
    rows = slab.shape[0]
    half = jax.ShapeDtypeStruct((PACKED, LANES), F32)
    whole = pl.BlockSpec((PACKED, LANES), lambda i, c: (0, 0))
    return pl.pallas_call(
        gram_kernel,
        out_shape=(half, half),
        grid_spec=pltpu.PrefetchScalarGridSpec(
            num_scalar_prefetch=1,
            grid=(rows // GRAM_ROWS,),
            in_specs=[pl.BlockSpec((GRAM_ROWS, N2), lambda i, c: (i, 0))],
            out_specs=(whole, whole),
            scratch_shapes=[pltpu.VMEM((2, PACKED, LANES), F32)],
        ),
        compiler_params=pltpu.CompilerParams(
            dimension_semantics=("arbitrary",), vmem_limit_bytes=48 << 20
        ),
        name="packed_gram",
    )(core, slab)


VMEM = pl.BlockSpec(memory_space=pltpu.VMEM)
SMEM = pl.BlockSpec(memory_space=pltpu.SMEM)


def join_kernel(parts_ref, out_ref):
    out_ref[...] = jnp.broadcast_to(jnp.sum(parts_ref[...], axis=0)[None], out_ref.shape)


def joined(parts):
    return pl.pallas_call(
        join_kernel,
        out_shape=jax.ShapeDtypeStruct(parts.shape, F32),
        in_specs=[VMEM],
        out_specs=VMEM,
        compiler_params=pltpu.CompilerParams(vmem_limit_bytes=12 << 20),
        name="join",
    )(parts)


def spread_kernel(start_ref, out_ref):
    pay = jnp.concatenate([start_ref[:, :LANES], start_ref[:, LANES:]], axis=0)
    out_ref[...] = jnp.broadcast_to(pay[None], out_ref.shape)


def spread(start):
    return pl.pallas_call(
        spread_kernel,
        out_shape=jax.ShapeDtypeStruct((CHIPS, 2 * START, LANES), F32),
        in_specs=[VMEM],
        out_specs=VMEM,
        compiler_params=pltpu.CompilerParams(vmem_limit_bytes=12 << 20),
        name="spread",
    )(start)


def eliminate(aug_ref):
    sub = lax.broadcasted_iota(jnp.int32, (8, LANES), 0)
    lane = lax.broadcasted_iota(jnp.int32, (1, LANES), 1)
    halves = GROUP // 8
    ones = jnp.ones((8, LANES), F32)
    for base in range(0, K, GROUP):
        first = base // LANES
        off = base % LANES
        tiles = range(first, first + 3)
        rows = [
            [aug_ref[base + 8 * v : base + 8 * v + 8, i * LANES : (i + 1) * LANES] for i in tiles]
            for v in range(halves)
        ]
        cols = [
            [jnp.broadcast_to(rows[v][0][:, off + t : off + t + 1], (8, LANES)) for t in range(GROUP)]
            for v in range(halves)
        ]
        inv = [ones for _ in range(halves)]
        for t in range(GROUP):
            vt, st = t // 8, t % 8
            pivot_col = [jnp.broadcast_to(cols[vt][s][st : st + 1], (8, LANES)) for s in range(t, GROUP)]
            pivot_row = [jnp.broadcast_to(r[st : st + 1], (8, LANES)) for r in rows[vt]]
            recip = 1.0 / pivot_col[0]
            inv[vt] = jnp.where(sub == st, recip, inv[vt])
            for v in range(vt, halves):
                mult = cols[v][t] * recip
                if v == vt:
                    mult = jnp.where(sub > st, mult, 0.0)
                for s in range(t + 1, GROUP):
                    cols[v][s] = cols[v][s] - mult * pivot_col[s - t]
                rows[v] = [r - mult * p for r, p in zip(rows[v], pivot_row)]
        upper = jnp.concatenate([jnp.concatenate(r, axis=1) for r in rows], axis=0)
        for v in range(halves):
            for i in range(first + 1):
                at = K + i * LANES
                aug_ref[base + 8 * v : base + 8 * v + 8, at : at + LANES] = rows[v][i + 2 - first] * jnp.sqrt(inv[v])
        if base + GROUP == K:
            break
        lower = jnp.concatenate(
            [jnp.concatenate([rows[v][i - first] * inv[v] for i in range(first, 2)], axis=1) for v in range(halves)],
            axis=0,
        )
        lh, lm, ll = split3(lower)
        uh, um, ul = split3(upper)
        left = jnp.concatenate([lh, lh, lm, lm, lh, ll], axis=0).T
        right = jnp.concatenate([uh, um, uh, um, ul, uh], axis=0)
        start = base + GROUP
        at = slice(first * LANES, (first + 3) * LANES)
        for lo, hi in ((start, start + GROUP), (start + GROUP, K)):
            if lo < hi:
                shift = first * LANES
                aug_ref[lo:hi, at] = aug_ref[lo:hi, at] - mm(left[lo - shift : hi - shift], right)


def passes_kernel(
    meta_ref, mine_ref, other_ref, start_mine_ref, start_other_ref,
    own_ref, basis_ref, gh_ref, gl_ref, aug_ref,
):
    core = meta_ref[0]
    slot = meta_ref[1]
    quarter = CHIPS // 2 * START

    def put(at_row, at_col, block):
        hi, lo = split2(block)
        rows = slice(at_row, at_row + block.shape[0])
        cols = slice(at_col, at_col + block.shape[1])
        gh_ref[rows, cols] = hi
        gl_ref[rows, cols] = lo

    def unpack(halves, starts):
        halves = [half[...].reshape(PACKED, LANES) for half in halves]
        for b in range(NB):
            row = BLK * b * (b + 1) // 2
            for a in range(b):
                for h, half in enumerate(halves):
                    block = half[row : row + BLK]
                    put(a * BLK, b * BLK + h * LANES, block)
                    put(b * BLK + h * LANES, a * BLK, block.T)
                row += BLK
            block = jnp.concatenate([half[row : row + BLK] for half in halves], axis=1)
            put(b * BLK, b * BLK, 0.5 * (block + block.T))
        for h, start in enumerate(starts):
            for half in range(2):
                chips = slice(half * CHIPS // 2, (half + 1) * CHIPS // 2)
                at = half * 2 * quarter + h * quarter
                for side in range(2):
                    rows = start[chips, side * START : (side + 1) * START, :]
                    basis_ref[at : at + quarter, side * LANES : (side + 1) * LANES] = rows.reshape(quarter, LANES)

    @pl.when(core == 0)
    def _():
        unpack((mine_ref, other_ref), (start_mine_ref, start_other_ref))

    @pl.when(core == 1)
    def _():
        unpack((other_ref, mine_ref), (start_other_ref, start_mine_ref))

    diag = lax.broadcasted_iota(jnp.int32, (K, K), 0) == lax.broadcasted_iota(jnp.int32, (K, K), 1)

    def one_pass(repeat, carry):
        bh, bl = split2(basis_ref[...])
        product = mm(gh_ref[...], bh) + (mm(gh_ref[...], bl) + mm(gl_ref[...], bh))
        aug_ref[:, :K] = mm6(product, product, TN)
        aug_ref[:, K:] = jnp.where(diag, 1.0, 0.0)
        eliminate(aug_ref)
        inverse = aug_ref[:, K:]
        basis_ref[...] = mm6(product, inverse, NT)
        return carry

    lax.fori_loop(0, PASSES, one_pass, 0)
    own_ref[...] = basis_ref[pl.ds(slot * START, START), :] * (float(N2) ** 0.5)


def passes(meta, *gathered):
    return pl.pallas_call(
        passes_kernel,
        out_shape=(
            jax.ShapeDtypeStruct((START, K), F32),
            jax.ShapeDtypeStruct((N2, K), F32),
        ),
        in_specs=[SMEM] + [VMEM] * 4,
        out_specs=(VMEM, VMEM),
        scratch_shapes=[
            pltpu.VMEM((N2, N2), BF16),
            pltpu.VMEM((N2, N2), BF16),
            pltpu.VMEM((K, 2 * K), F32),
        ],
        compiler_params=pltpu.CompilerParams(vmem_limit_bytes=30 << 20),
        name="passes",
    )(meta, *gathered)


def core_kernel(slab_ref, basis_ref, out_ref):
    out_ref[...] = mm3(slab_ref[...], basis_ref[...])


def core_block(slab, basis):
    rows = slab.shape[0]
    return pl.pallas_call(
        core_kernel,
        out_shape=jax.ShapeDtypeStruct((rows, K), F32),
        grid=(rows // CORE_ROWS,),
        in_specs=[
            pl.BlockSpec((CORE_ROWS, N2), lambda i: (i, 0)),
            pl.BlockSpec((N2, K), lambda i: (0, 0)),
        ],
        out_specs=pl.BlockSpec((CORE_ROWS, K), lambda i: (i, 0)),
        compiler_params=pltpu.CompilerParams(
            dimension_semantics=("arbitrary",), vmem_limit_bytes=48 << 20
        ),
        name="core_block",
    )(slab, basis)


CHIP_AXES = ("zhi", "zlo", "y", "x")


def swap_cores(x):
    return lax.ppermute(x, "core", [(0, 1), (1, 0)])


def exchange(x):
    return lax.all_to_all(x, CHIP_AXES, split_axis=0, concat_axis=0)


def body(tensor, start_basis):
    core = lax.axis_index("core")
    col = (lax.axis_index("zlo") * 4 + lax.axis_index("y")) * 4 + lax.axis_index("x")
    slot = (lax.axis_index("zhi") * 2 + core) * 32 + col
    slab = tensor.reshape(-1, N2)
    start_mine = exchange(spread(start_basis))
    keep, send = packed_gram(core.reshape(1), slab)
    keep, send, start_mine = lax.optimization_barrier((keep, send, start_mine))
    chip = (keep + swap_cores(send)).reshape(CHIPS, OWN, LANES)
    mine = exchange(joined(exchange(chip)))
    own, basis = passes(
        jnp.stack([core, slot]), mine, swap_cores(mine), start_mine, swap_cores(start_mine)
    )
    core_out = core_block(slab, basis)
    return own, core_out.reshape(tensor.shape[0], tensor.shape[1], K)


def solution(mesh):
    split = Mesh(mesh.devices.reshape(2, 2, 2, 4, 4), ("zhi", "core", "zlo", "y", "x"))
    row, col = ("zhi", "core"), ("zlo", "y", "x")
    return jax.shard_map(
        body,
        mesh=split,
        in_specs=(P(row, col, None), P(row + col, None)),
        out_specs=(P(row + col, None), P(row, col, None)),
        check_vma=False,
    )
```

```python
import jax
import jax.numpy as jnp
from jax import lax
from jax.experimental import pallas as pl
from jax.experimental.pallas import tpu as pltpu
from jax.sharding import Mesh
from jax.sharding import PartitionSpec as P

PASSES = 2
N2 = 1024
K = 256
BLK = 256
NB = N2 // BLK
PACKED = BLK * NB * (NB + 1) // 2
LANES = 128
CHIPS = 64
OWN = PACKED // CHIPS
START = 8
PAY = OWN + 2 * START
GRAM_ROWS = 512
CORE_ROWS = 1024
GROUP = 32
CHUNK = 256
F32 = jnp.float32
BF16 = jnp.bfloat16
NN = (((1,), (0,)), ((), ()))
NT = (((1,), (1,)), ((), ()))
TN = (((0,), (0,)), ((), ()))


def mm(a, b, dims=NN):
    return lax.dot_general(a, b, dims, preferred_element_type=F32)


def split2(x):
    hi = x.astype(BF16)
    return hi, (x - hi.astype(F32)).astype(BF16)


def split3(x):
    hi = x.astype(BF16)
    rest = x - hi.astype(F32)
    mid = rest.astype(BF16)
    return hi, mid, (rest - mid.astype(F32)).astype(BF16)


def gram_kernel(core_ref, slab_ref, keep_ref, send_ref, acc_ref):
    step = pl.program_id(0)

    @pl.when(step == 0)
    def _():
        acc_ref[...] = jnp.zeros_like(acc_ref)

    hi, lo = split2(slab_ref[...])
    hi_t, lo_t = hi.T, lo.T
    for b in range(NB):
        cols = slice(b * BLK, (b + 1) * BLK)
        hb, lb = hi[:, cols], lo[:, cols]
        top = b * BLK
        row = BLK * b * (b + 1) // 2
        for a in range(0, top, BLK):
            part = mm(hi_t[a : a + BLK], hb) + mm(hi_t[a : a + BLK], lb) + mm(lo_t[a : a + BLK], hb)
            acc_ref[0, row + a : row + a + BLK] += part[:, :LANES]
            acc_ref[1, row + a : row + a + BLK] += part[:, LANES:]
        part = mm(hi_t[cols], hb) + mm(hi_t[cols], lb + lb)
        acc_ref[0, row + top : row + top + BLK] += part[:, :LANES]
        acc_ref[1, row + top : row + top + BLK] += part[:, LANES:]

    @pl.when(step == pl.num_programs(0) - 1)
    def _():
        core = core_ref[0]
        keep_ref[...] = acc_ref[core]
        send_ref[...] = acc_ref[1 - core]


def packed_gram(core, slab):
    rows = slab.shape[0]
    half = jax.ShapeDtypeStruct((PACKED, LANES), F32)
    whole = pl.BlockSpec((PACKED, LANES), lambda i, c: (0, 0))
    return pl.pallas_call(
        gram_kernel,
        out_shape=(half, half),
        grid_spec=pltpu.PrefetchScalarGridSpec(
            num_scalar_prefetch=1,
            grid=(rows // GRAM_ROWS,),
            in_specs=[pl.BlockSpec((GRAM_ROWS, N2), lambda i, c: (i, 0))],
            out_specs=(whole, whole),
            scratch_shapes=[pltpu.VMEM((2, PACKED, LANES), F32)],
        ),
        compiler_params=pltpu.CompilerParams(
            dimension_semantics=("arbitrary",), vmem_limit_bytes=48 << 20
        ),
        name="packed_gram",
    )(core, slab)


def join_kernel(parts_ref, start_ref, out_ref):
    total = jnp.sum(parts_ref[...], axis=0)
    pay = jnp.concatenate([total, start_ref[:, :LANES], start_ref[:, LANES:]], axis=0)
    out_ref[...] = jnp.broadcast_to(pay[None], out_ref.shape)


def joined(parts, start):
    return pl.pallas_call(
        join_kernel,
        out_shape=jax.ShapeDtypeStruct((CHIPS, PAY, LANES), F32),
        name="join",
    )(parts, start)


def eliminate(aug_ref):
    sub = lax.broadcasted_iota(jnp.int32, (8, LANES), 0)
    halves = GROUP // 8
    ones = jnp.ones((8, LANES), F32)
    for base in range(0, K, GROUP):
        first = base // LANES
        off = base % LANES
        tiles = range(first, first + 3)
        rows = [
            [aug_ref[base + 8 * v : base + 8 * v + 8, i * LANES : (i + 1) * LANES] for i in tiles]
            for v in range(halves)
        ]
        cols = [
            [jnp.broadcast_to(rows[v][0][:, off + t : off + t + 1], (8, LANES)) for t in range(GROUP)]
            for v in range(halves)
        ]
        inv = [ones for _ in range(halves)]
        for t in range(GROUP):
            vt, st = t // 8, t % 8
            pivot_row = [jnp.broadcast_to(r[st : st + 1], (8, LANES)) for r in rows[vt]]
            recip = 1.0 / jnp.broadcast_to(cols[vt][t][st : st + 1], (8, LANES))
            inv[vt] = jnp.where(sub == st, recip, inv[vt])
            mult = {}
            for v in range(vt, halves):
                m = cols[v][t] * recip
                mult[v] = jnp.where(sub > st, m, 0.0) if v == vt else m
                rows[v] = [r - mult[v] * p for r, p in zip(rows[v], pivot_row)]
            for s in range(t + 1, GROUP):
                entry = jnp.broadcast_to(cols[s // 8][t][s % 8 : s % 8 + 1], (8, LANES))
                for v in range(s // 8, halves):
                    cols[v][s] = cols[v][s] - mult[v] * entry
        upper = jnp.concatenate([jnp.concatenate(r, axis=1) for r in rows], axis=0)
        for v in range(halves):
            for i in range(first + 1):
                at = K + i * LANES
                aug_ref[base + 8 * v : base + 8 * v + 8, at : at + LANES] = rows[v][i + 2 - first] * jnp.sqrt(inv[v])
        if base + GROUP == K:
            break
        lower = jnp.concatenate(
            [jnp.concatenate([rows[v][i - first] * inv[v] for i in range(first, 2)], axis=1) for v in range(halves)],
            axis=0,
        )
        lh, lm, ll = split3(lower)
        uh, um, ul = split3(upper)
        left = jnp.concatenate([lh, lh, lm, lm, lh, ll], axis=0).T
        right = jnp.concatenate([uh, um, uh, um, ul, uh], axis=0)
        start = base + GROUP
        at = slice(first * LANES, (first + 3) * LANES)
        for lo, hi in ((start, start + GROUP), (start + GROUP, K)):
            if lo < hi:
                shift = first * LANES
                aug_ref[lo:hi, at] = aug_ref[lo:hi, at] - mm(left[lo - shift : hi - shift], right)


def passes_kernel(meta_ref, mine_ref, other_ref, own_ref, basis_ref, gh_ref, gl_ref, aug_ref, bh_ref, bl_ref, ph_ref, pm_ref):
    core = meta_ref[0]
    slot = meta_ref[1]
    quarter = CHIPS // 2 * START

    def place(h, ref):
        packed = ref[:, :OWN, :].reshape(PACKED, LANES)
        for b in range(NB):
            for a in range(b):
                row = BLK * (b * (b + 1) // 2 + a)
                block = packed[row : row + BLK]
                hi, lo = split2(block)
                at = b * BLK + h * LANES
                gh_ref[a * BLK : (a + 1) * BLK, at : at + LANES] = hi
                gl_ref[a * BLK : (a + 1) * BLK, at : at + LANES] = lo
                hi, lo = split2(block.T)
                gh_ref[at : at + LANES, a * BLK : (a + 1) * BLK] = hi
                gl_ref[at : at + LANES, a * BLK : (a + 1) * BLK] = lo

    def place_diagonal(left, right):
        for b in range(NB):
            row = BLK * (b * (b + 1) // 2 + b)
            block = jnp.concatenate(
                [r[:, :OWN, :].reshape(PACKED, LANES)[row : row + BLK] for r in (left, right)], axis=1
            )
            hi, lo = split2(0.5 * (block + block.T))
            at = slice(b * BLK, (b + 1) * BLK)
            gh_ref[at, at] = hi
            gl_ref[at, at] = lo

    def place_start(h, ref):
        for half in range(2):
            chips = slice(half * CHIPS // 2, (half + 1) * CHIPS // 2)
            at = half * 2 * quarter + h * quarter
            for side in range(2):
                rows = ref[chips, OWN + side * START : OWN + (side + 1) * START, :]
                basis_ref[at : at + quarter, side * LANES : (side + 1) * LANES] = rows.reshape(quarter, LANES)

    def unpack(left, right):
        for h, ref in enumerate((left, right)):
            place(h, ref)
            place_start(h, ref)
        place_diagonal(left, right)

    @pl.when(core == 0)
    def _():
        unpack(mine_ref, other_ref)

    @pl.when(core == 1)
    def _():
        unpack(other_ref, mine_ref)

    diag = lax.broadcasted_iota(jnp.int32, (K, K), 0) == lax.broadcasted_iota(jnp.int32, (K, K), 1)

    bh_ref[...], bl_ref[...] = split2(basis_ref[...])

    def one_pass(repeat, carry):
        even = cross = jnp.zeros((K, K), F32)
        for at in range(0, N2, CHUNK):
            rows = slice(at, at + CHUNK)
            bh = bh_ref[...]
            product = mm(gh_ref[rows], bh) + (mm(gh_ref[rows], bl_ref[...]) + mm(gl_ref[rows], bh))
            high, mid, low = split3(product)
            ph_ref[rows] = high
            pm_ref[rows] = mid
            high_t, mid_t = high.T, mid.T
            even += mm(high_t, high) + mm(mid_t, mid)
            cross += mm(high_t, mid) + mm(high_t, low)
        aug_ref[:, :K] = even + (cross + cross.T)
        aug_ref[:, K:] = jnp.where(diag, 1.0, 0.0)
        eliminate(aug_ref)
        ih, il = split2(aug_ref[:, K:].T)
        for at in range(0, N2, CHUNK):
            rows = slice(at, at + CHUNK)
            part = mm(ph_ref[rows], ih) + (mm(ph_ref[rows], il) + mm(pm_ref[rows], ih))
            basis_ref[rows] = part
            bh_ref[rows], bl_ref[rows] = split2(part)
        return carry

    lax.fori_loop(0, PASSES, one_pass, 0)
    own_ref[...] = basis_ref[pl.ds(slot * START, START), :] * (float(N2) ** 0.5)


def passes(meta, mine, other):
    vmem = pl.BlockSpec(memory_space=pltpu.VMEM)
    return pl.pallas_call(
        passes_kernel,
        out_shape=(
            jax.ShapeDtypeStruct((START, K), F32),
            jax.ShapeDtypeStruct((N2, K), F32),
        ),
        in_specs=[pl.BlockSpec(memory_space=pltpu.SMEM), vmem, vmem],
        out_specs=(vmem, vmem),
        scratch_shapes=[
            pltpu.VMEM((N2, N2), BF16),
            pltpu.VMEM((N2, N2), BF16),
            pltpu.VMEM((K, 2 * K), F32),
            pltpu.VMEM((N2, K), BF16),
            pltpu.VMEM((N2, K), BF16),
            pltpu.VMEM((N2, K), BF16),
            pltpu.VMEM((N2, K), BF16),
        ],
        compiler_params=pltpu.CompilerParams(vmem_limit_bytes=48 << 20),
        name="passes",
    )(meta, mine, other)


def core_kernel(slab_ref, basis_ref, out_ref):
    sh, sl = split2(basis_ref[...])
    for at in range(0, CORE_ROWS, CHUNK):
        hi, lo = split2(slab_ref[at : at + CHUNK])
        out_ref[at : at + CHUNK] = mm(hi, sh) + (mm(hi, sl) + mm(lo, sh))


def core_block(slab, basis):
    rows = slab.shape[0]
    return pl.pallas_call(
        core_kernel,
        out_shape=jax.ShapeDtypeStruct((rows, K), F32),
        grid=(rows // CORE_ROWS,),
        in_specs=[
            pl.BlockSpec((CORE_ROWS, N2), lambda i: (i, 0)),
            pl.BlockSpec((N2, K), lambda i: (0, 0)),
        ],
        out_specs=pl.BlockSpec((CORE_ROWS, K), lambda i: (i, 0)),
        compiler_params=pltpu.CompilerParams(
            dimension_semantics=("arbitrary",), vmem_limit_bytes=48 << 20
        ),
        name="core_block",
    )(slab, basis)


CHIP_AXES = ("zhi", "zlo", "y", "x")


def swap_cores(x):
    return lax.ppermute(x, "core", [(0, 1), (1, 0)])


def exchange(x):
    return lax.all_to_all(x, CHIP_AXES, split_axis=0, concat_axis=0)


def body(tensor, start_basis):
    core = lax.axis_index("core")
    col = (lax.axis_index("zlo") * 4 + lax.axis_index("y")) * 4 + lax.axis_index("x")
    slot = (lax.axis_index("zhi") * 2 + core) * 32 + col
    slab = tensor.reshape(-1, N2)
    keep, send = packed_gram(core.reshape(1), slab)
    chip = (keep + swap_cores(send)).reshape(CHIPS, OWN, LANES)
    mine = exchange(joined(exchange(chip), start_basis))
    own, basis = passes(jnp.stack([core, slot]), mine, swap_cores(mine))
    core_out = core_block(slab, basis)
    return own, core_out.reshape(tensor.shape[0], tensor.shape[1], K)


def solution(mesh):
    split = Mesh(mesh.devices.reshape(2, 2, 2, 4, 4), ("zhi", "core", "zlo", "y", "x"))
    row, col = ("zhi", "core"), ("zlo", "y", "x")
    return jax.shard_map(
        body,
        mesh=split,
        in_specs=(P(row, col, None), P(row + col, None)),
        out_specs=(P(row + col, None), P(row, col, None)),
        check_vma=False,
    )
```

```python
import jax
import jax.numpy as jnp
from jax import lax
from jax.experimental import pallas as pl
from jax.experimental.pallas import tpu as pltpu
from jax.sharding import Mesh
from jax.sharding import PartitionSpec as P

PASSES = 2
N2 = 1024
K = 256
BLK = 256
NB = N2 // BLK
PACKED = BLK * NB * (NB + 1) // 2
LANES = 128
CHIPS = 64
OWN = PACKED // CHIPS
START = 8
PAY = OWN + 2 * START
GRAM_ROWS = 512
CORE_ROWS = 1024
GROUP = 32
CHUNK = 256
F32 = jnp.float32
BF16 = jnp.bfloat16
NN = (((1,), (0,)), ((), ()))
NT = (((1,), (1,)), ((), ()))
TN = (((0,), (0,)), ((), ()))


def mm(a, b, dims=NN):
    return lax.dot_general(a, b, dims, preferred_element_type=F32)


def split2(x):
    hi = x.astype(BF16)
    return hi, (x - hi.astype(F32)).astype(BF16)


def split3(x):
    hi = x.astype(BF16)
    rest = x - hi.astype(F32)
    mid = rest.astype(BF16)
    return hi, mid, (rest - mid.astype(F32)).astype(BF16)


def gram_kernel(core_ref, slab_ref, keep_ref, send_ref, acc_ref):
    step = pl.program_id(0)

    @pl.when(step == 0)
    def _():
        acc_ref[...] = jnp.zeros_like(acc_ref)

    hi, lo = split2(slab_ref[...])
    hi_t, lo_t = hi.T, lo.T
    for b in range(NB):
        cols = slice(b * BLK, (b + 1) * BLK)
        hb, lb = hi[:, cols], lo[:, cols]
        top = b * BLK
        row = BLK * b * (b + 1) // 2
        for a in range(0, top, BLK):
            part = mm(hi_t[a : a + BLK], hb) + mm(hi_t[a : a + BLK], lb) + mm(lo_t[a : a + BLK], hb)
            acc_ref[0, row + a : row + a + BLK] += part[:, :LANES]
            acc_ref[1, row + a : row + a + BLK] += part[:, LANES:]
        part = mm(hi_t[cols], hb) + mm(hi_t[cols], lb + lb)
        acc_ref[0, row + top : row + top + BLK] += part[:, :LANES]
        acc_ref[1, row + top : row + top + BLK] += part[:, LANES:]

    @pl.when(step == pl.num_programs(0) - 1)
    def _():
        core = core_ref[0]
        keep_ref[...] = acc_ref[core]
        send_ref[...] = acc_ref[1 - core]


def packed_gram(core, slab):
    rows = slab.shape[0]
    half = jax.ShapeDtypeStruct((PACKED, LANES), F32)
    whole = pl.BlockSpec((PACKED, LANES), lambda i, c: (0, 0))
    return pl.pallas_call(
        gram_kernel,
        out_shape=(half, half),
        grid_spec=pltpu.PrefetchScalarGridSpec(
            num_scalar_prefetch=1,
            grid=(rows // GRAM_ROWS,),
            in_specs=[pl.BlockSpec((GRAM_ROWS, N2), lambda i, c: (i, 0))],
            out_specs=(whole, whole),
            scratch_shapes=[pltpu.VMEM((2, PACKED, LANES), F32)],
        ),
        compiler_params=pltpu.CompilerParams(
            dimension_semantics=("arbitrary",), vmem_limit_bytes=48 << 20
        ),
        name="packed_gram",
    )(core, slab)


VMEM = pl.BlockSpec(memory_space=pltpu.VMEM)
SMEM = pl.BlockSpec(memory_space=pltpu.SMEM)
HBM = pl.BlockSpec(memory_space=pl.ANY)


def join_kernel(parts_ref, start_ref, out_ref):
    total = jnp.sum(parts_ref[...], axis=0)
    pay = jnp.concatenate([total, start_ref[:, :LANES], start_ref[:, LANES:]], axis=0)
    out_ref[...] = jnp.broadcast_to(pay[None], out_ref.shape)


def joined(parts, start):
    return pl.pallas_call(
        join_kernel,
        out_shape=jax.ShapeDtypeStruct((CHIPS, PAY, LANES), F32),
        in_specs=[VMEM, VMEM],
        out_specs=VMEM,
        compiler_params=pltpu.CompilerParams(vmem_limit_bytes=12 << 20),
        name="join",
    )(parts, start)


def eliminate(aug_ref):
    sub = lax.broadcasted_iota(jnp.int32, (8, LANES), 0)
    halves = GROUP // 8
    ones = jnp.ones((8, LANES), F32)
    for base in range(0, K, GROUP):
        first = base // LANES
        off = base % LANES
        tiles = range(first, first + 3)
        rows = [
            [aug_ref[base + 8 * v : base + 8 * v + 8, i * LANES : (i + 1) * LANES] for i in tiles]
            for v in range(halves)
        ]
        cols = [
            [jnp.broadcast_to(rows[v][0][:, off + t : off + t + 1], (8, LANES)) for t in range(GROUP)]
            for v in range(halves)
        ]
        inv = [ones for _ in range(halves)]
        for t in range(GROUP):
            vt, st = t // 8, t % 8
            pivot_row = [jnp.broadcast_to(r[st : st + 1], (8, LANES)) for r in rows[vt]]
            recip = 1.0 / jnp.broadcast_to(cols[vt][t][st : st + 1], (8, LANES))
            inv[vt] = jnp.where(sub == st, recip, inv[vt])
            mult = {}
            for v in range(vt, halves):
                m = cols[v][t] * recip
                mult[v] = jnp.where(sub > st, m, 0.0) if v == vt else m
                rows[v] = [r - mult[v] * p for r, p in zip(rows[v], pivot_row)]
            for s in range(t + 1, GROUP):
                entry = jnp.broadcast_to(cols[s // 8][t][s % 8 : s % 8 + 1], (8, LANES))
                for v in range(s // 8, halves):
                    cols[v][s] = cols[v][s] - mult[v] * entry
        upper = jnp.concatenate([jnp.concatenate(r, axis=1) for r in rows], axis=0)
        for v in range(halves):
            for i in range(first + 1):
                at = K + i * LANES
                aug_ref[base + 8 * v : base + 8 * v + 8, at : at + LANES] = rows[v][i + 2 - first] * jnp.sqrt(inv[v])
        if base + GROUP == K:
            break
        lower = jnp.concatenate(
            [jnp.concatenate([rows[v][i - first] * inv[v] for i in range(first, 2)], axis=1) for v in range(halves)],
            axis=0,
        )
        lh, lm, ll = split3(lower)
        uh, um, ul = split3(upper)
        left = jnp.concatenate([lh, lh, lm, lm, lh, ll], axis=0).T
        right = jnp.concatenate([uh, um, uh, um, ul, uh], axis=0)
        start = base + GROUP
        at = slice(first * LANES, (first + 3) * LANES)
        for lo, hi in ((start, start + GROUP), (start + GROUP, K)):
            if lo < hi:
                shift = first * LANES
                aug_ref[lo:hi, at] = aug_ref[lo:hi, at] - mm(left[lo - shift : hi - shift], right)


def passes_kernel(
    meta_ref, mine_ref, other_ref, slab_hbm,
    own_ref, core_hbm,
    slab_ref, out_ref, basis_ref, gh_ref, gl_ref, aug_ref, bh_ref, bl_ref, ph_ref, pm_ref, in_sems, out_sems,
):
    core = meta_ref[0]
    slot = meta_ref[1]
    steps = slab_hbm.shape[0] // CORE_ROWS

    def load(step):
        rows = slice(step * CORE_ROWS, (step + 1) * CORE_ROWS)
        return pltpu.make_async_copy(slab_hbm.at[rows], slab_ref.at[rows], in_sems.at[step])

    def store(step):
        rows = slice(step * CORE_ROWS, (step + 1) * CORE_ROWS)
        return pltpu.make_async_copy(out_ref.at[rows], core_hbm.at[rows], out_sems.at[step])

    for step in range(steps):
        load(step).start()
    quarter = CHIPS // 2 * START

    def place(h, ref):
        packed = ref[:, :OWN, :].reshape(PACKED, LANES)
        for b in range(NB):
            for a in range(b):
                row = BLK * (b * (b + 1) // 2 + a)
                block = packed[row : row + BLK]
                hi, lo = split2(block)
                at = b * BLK + h * LANES
                gh_ref[a * BLK : (a + 1) * BLK, at : at + LANES] = hi
                gl_ref[a * BLK : (a + 1) * BLK, at : at + LANES] = lo
                hi, lo = split2(block.T)
                gh_ref[at : at + LANES, a * BLK : (a + 1) * BLK] = hi
                gl_ref[at : at + LANES, a * BLK : (a + 1) * BLK] = lo

    def place_diagonal(left, right):
        for b in range(NB):
            row = BLK * (b * (b + 1) // 2 + b)
            block = jnp.concatenate(
                [r[:, :OWN, :].reshape(PACKED, LANES)[row : row + BLK] for r in (left, right)], axis=1
            )
            hi, lo = split2(0.5 * (block + block.T))
            at = slice(b * BLK, (b + 1) * BLK)
            gh_ref[at, at] = hi
            gl_ref[at, at] = lo

    def place_start(h, ref):
        for half in range(2):
            chips = slice(half * CHIPS // 2, (half + 1) * CHIPS // 2)
            at = half * 2 * quarter + h * quarter
            for side in range(2):
                rows = ref[chips, OWN + side * START : OWN + (side + 1) * START, :]
                basis_ref[at : at + quarter, side * LANES : (side + 1) * LANES] = rows.reshape(quarter, LANES)

    def unpack(left, right):
        for h, ref in enumerate((left, right)):
            place(h, ref)
            place_start(h, ref)
        place_diagonal(left, right)

    @pl.when(core == 0)
    def _():
        unpack(mine_ref, other_ref)

    @pl.when(core == 1)
    def _():
        unpack(other_ref, mine_ref)

    diag = lax.broadcasted_iota(jnp.int32, (K, K), 0) == lax.broadcasted_iota(jnp.int32, (K, K), 1)

    bh_ref[...], bl_ref[...] = split2(basis_ref[...])

    def one_pass(repeat, carry):
        even = cross = jnp.zeros((K, K), F32)
        for at in range(0, N2, CHUNK):
            rows = slice(at, at + CHUNK)
            bh = bh_ref[...]
            product = mm(gh_ref[rows], bh) + (mm(gh_ref[rows], bl_ref[...]) + mm(gl_ref[rows], bh))
            high, mid, low = split3(product)
            ph_ref[rows] = high
            pm_ref[rows] = mid
            high_t, mid_t = high.T, mid.T
            even += mm(high_t, high) + mm(mid_t, mid)
            cross += mm(high_t, mid) + mm(high_t, low)
        aug_ref[:, :K] = even + (cross + cross.T)
        aug_ref[:, K:] = jnp.where(diag, 1.0, 0.0)
        eliminate(aug_ref)
        ih, il = split2(aug_ref[:, K:].T)
        for at in range(0, N2, CHUNK):
            rows = slice(at, at + CHUNK)
            part = mm(ph_ref[rows], ih) + (mm(ph_ref[rows], il) + mm(pm_ref[rows], ih))
            basis_ref[rows] = part
            bh_ref[rows], bl_ref[rows] = split2(part)
        return carry

    lax.fori_loop(0, PASSES, one_pass, 0)
    own_ref[...] = basis_ref[pl.ds(slot * START, START), :] * (float(N2) ** 0.5)
    for step in range(steps):
        load(step).wait()
        for at in range(step * CORE_ROWS, (step + 1) * CORE_ROWS, CHUNK):
            rows = slice(at, at + CHUNK)
            hi, lo = split2(slab_ref[rows])
            out_ref[rows] = mm(hi, bh_ref[...]) + (mm(hi, bl_ref[...]) + mm(lo, bh_ref[...]))
        store(step).start()
    for step in range(steps):
        store(step).wait()


def passes(meta, mine, other, slab):
    rows = slab.shape[0]
    steps = rows // CORE_ROWS
    return pl.pallas_call(
        passes_kernel,
        out_shape=(
            jax.ShapeDtypeStruct((START, K), F32),
            jax.ShapeDtypeStruct((rows, K), F32),
        ),
        in_specs=[SMEM, VMEM, VMEM, HBM],
        out_specs=(VMEM, HBM),
        scratch_shapes=[
            pltpu.VMEM((rows, N2), F32),
            pltpu.VMEM((rows, K), F32),
            pltpu.VMEM((N2, K), F32),
            pltpu.VMEM((N2, N2), BF16),
            pltpu.VMEM((N2, N2), BF16),
            pltpu.VMEM((K, 2 * K), F32),
            pltpu.VMEM((N2, K), BF16),
            pltpu.VMEM((N2, K), BF16),
            pltpu.VMEM((N2, K), BF16),
            pltpu.VMEM((N2, K), BF16),
            pltpu.SemaphoreType.DMA((steps,)),
            pltpu.SemaphoreType.DMA((steps,)),
        ],
        compiler_params=pltpu.CompilerParams(vmem_limit_bytes=48 << 20),
        name="passes",
    )(meta, mine, other, slab)


CHIP_AXES = ("zhi", "zlo", "y", "x")


def swap_cores(x):
    return lax.ppermute(x, "core", [(0, 1), (1, 0)])


def exchange(x):
    return lax.all_to_all(x, CHIP_AXES, split_axis=0, concat_axis=0)


def body(tensor, start_basis):
    core = lax.axis_index("core")
    col = (lax.axis_index("zlo") * 4 + lax.axis_index("y")) * 4 + lax.axis_index("x")
    slot = (lax.axis_index("zhi") * 2 + core) * 32 + col
    slab = tensor.reshape(-1, N2)
    keep, send = packed_gram(core.reshape(1), slab)
    chip = (keep + swap_cores(send)).reshape(CHIPS, OWN, LANES)
    mine = exchange(joined(exchange(chip), start_basis))
    own, core_out = passes(jnp.stack([core, slot]), mine, swap_cores(mine), slab)
    return own, core_out.reshape(tensor.shape[0], tensor.shape[1], K)


def solution(mesh):
    split = Mesh(mesh.devices.reshape(2, 2, 2, 4, 4), ("zhi", "core", "zlo", "y", "x"))
    row, col = ("zhi", "core"), ("zlo", "y", "x")
    return jax.shard_map(
        body,
        mesh=split,
        in_specs=(P(row, col, None), P(row + col, None)),
        out_specs=(P(row + col, None), P(row, col, None)),
        check_vma=False,
    )
```
